256 devices in a mesh: dp: 64 (over y, x_hi, z), mp: 4 (over x_lo, core).
Axes of the slice: x: 4 (x_hi: 2, x_lo: 2; x = x_hi * 2 + x_lo), y: 4, z: 8, core: 2. Of those that a mesh axis runs over, the one named last changes fastest.
Arguments:
- picture_skip_activations: bfloat16 [131072, 1152], P('dp'), as said below
- caption_closing_activations: bfloat16 [512, 1152], P('dp'), as said below
- normaliser_multipliers: float32 [3, 1152], replicated, may hold values from 0.1 to 1.9
- widening_matrix: bfloat16 [1152, 4304], P('dp', 'mp'), may hold values from -0.1875 to 0.1875
- contracting_matrix: bfloat16 [4304, 1152], P('mp', 'dp'), as said below
- caption_mapping_matrix: bfloat16 [1152, 1152], replicated, as said below
- sharpness_factor: float32 [1], replicated, may hold values from 8 to 32
- score_offset_term: float32 [1], replicated, may hold values from -8 to -3
Outputs:
- row_loss: float32 [512], P('dp')
- col_loss: float32 [512], P('dp')
The draws below stay inside these ranges and needn't reach their ends.
Inputs may be any that keep to these rules, and one draw needn't show every extreme that they name: `picture_skip_activations`: entries lie within -8 and 8. `caption_closing_activations`: entries lie within -8 and 8. `contracting_matrix`: entries are at most 4.4 / sqrt(4304) in magnitude. `caption_mapping_matrix`: diagonal entries lie within 1 - 2.1 / sqrt(1152) and 1 + 2.1 / sqrt(1152), the others within -2.1 / sqrt(1152) and 2.1 / sqrt(1152).
All inputs are finite; a program needn't handle non-finite values.
Results may differ from the reference program's by a relative error of at most 0.01.
Values may be sent and summed in bfloat16 or wider, within the bound.
No kernel may reach another device: no remote copies, remote signals or barrier semaphores. Data moves between devices by JAX's collectives and lax.ppermute only.
A program may use at most 128 MiB of HBM per device.

```python
import math
import jax
import jax.numpy as jnp
from jax import lax

D = 1152
MLP = 4304
PATCHES = 256
IMG_DEV = 8
PAIRS = 512
N_DP = 64
N_MP = 4


latent_rank = 16


offset_amplitude = 1.5


direction_weight = 1.33


skip_spread = 0.8


head_spread = 0.7


def shared_direction(key):
    sign_table = jnp.where(jnp.arange(D) < D // 2, 1.0, -1.0).astype(jnp.float32)
    return jax.random.permutation(jax.random.fold_in(key, 101), sign_table)


def pair_offsets(key):
    latent = jax.random.normal(jax.random.fold_in(key, 202), (PAIRS, latent_rank), jnp.float32)
    basis_rows = jax.random.normal(jax.random.fold_in(key, 203), (latent_rank, D), jnp.float32) * latent_rank ** (-0.5)
    return offset_amplitude * jnp.dot(latent, basis_rows, precision=lax.Precision.HIGHEST)


def draw_picture_skip_activations(key, part):
    direction = shared_direction(key)
    offsets = pair_offsets(key)
    noise_key = jax.random.fold_in(key, 301)
    field_shape = (PAIRS, PATCHES, D)
    noise_part = jax.random.truncated_normal(noise_key, -4.5, 4.5, field_shape, jnp.float32)
    along_axis = skip_spread * jax.random.truncated_normal(jax.random.fold_in(key, 302), -3.0, 3.0, (PAIRS, PATCHES, 1), jnp.float32)
    field_sum = noise_part + offsets[:, None, :] + along_axis * direction[None, None, :]
    return jnp.clip(field_sum, -8.0, 8.0).reshape(PAIRS * PATCHES, D).astype(jnp.bfloat16)


def draw_caption_closing_activations(key, part):
    offsets = pair_offsets(key)
    noise_key = jax.random.fold_in(key, 401)
    noise_part = jax.random.truncated_normal(noise_key, -4.5, 4.5, (PAIRS, D), jnp.float32)
    return jnp.clip(noise_part + offsets, -8.0, 8.0).astype(jnp.bfloat16)


def draw_contracting_matrix(key, part):
    direction = shared_direction(key)
    sign_table = jnp.where(jnp.arange(MLP) < MLP // 2, 1.0, -1.0).astype(jnp.float32)
    unit_signs = jax.random.permutation(jax.random.fold_in(key, 501), sign_table)
    noise_key = jax.random.fold_in(key, 502)
    noise_part = jax.random.truncated_normal(noise_key, -3.0, 3.0, (MLP, D), jnp.float32)
    weights = (direction_weight * unit_signs[:, None] * direction[None, :] + noise_part) * MLP ** (-0.5)
    return weights.astype(jnp.bfloat16)


def draw_caption_mapping_matrix(key, part):
    noise_key = jax.random.fold_in(key, 601)
    noise_part = jax.random.truncated_normal(noise_key, -3.0, 3.0, (D, D), jnp.float32)
    return (jnp.eye(D, dtype=jnp.float32) + head_spread * D ** (-0.5) * noise_part).astype(jnp.bfloat16)


def steps_of(key, extent, cuts, smallest, top_value):
    gain, own = 1.0, jax.random.fold_in(key, 6)
    for position, parts in cuts:
        steps = jnp.exp(jax.random.uniform(jax.random.fold_in(own, position), (parts,), jnp.float32, smallest / len(cuts), top_value / len(cuts)))
        gain = gain * jnp.repeat(steps, extent[position] // parts).reshape([-1 if axis == position else 1 for axis in range(len(extent))])
    return gain


def bell_draw(stream_key, dims, scale, most, shards=(), kind=jnp.bfloat16):
    array = jax.random.normal(stream_key, dims, jnp.float32) * scale
    if len(shards) > 0:
        array = steps_of(stream_key, dims, shards, -0.22, 0.18) * array
    return jnp.clip(array, min=-most, max=most).astype(kind)


def setup_inputs(seed: int = 0) -> dict:
    seeds = jax.random.split(jax.random.key(seed), 9)
    return {
        "picture_skip_activations": draw_picture_skip_activations(jax.random.fold_in(seeds[8], 71), 0),
        "caption_closing_activations": draw_caption_closing_activations(jax.random.fold_in(seeds[8], 71), 0),
        "normaliser_multipliers": jnp.clip(1.0 + 0.18 * jax.random.normal(seeds[2], (3, D), jnp.float32), 0.1, 1.9),
        "widening_matrix": bell_draw(seeds[3], (D, MLP), D ** -0.5, 0.1875, ((0, 64), (1, 4))),
        "contracting_matrix": draw_contracting_matrix(jax.random.fold_in(seeds[8], 71), 0),
        "caption_mapping_matrix": draw_caption_mapping_matrix(jax.random.fold_in(seeds[8], 71), 0),
        "sharpness_factor": jnp.clip(jnp.exp(jax.random.uniform(seeds[6], (1,), jnp.float32, math.log(8.0), math.log(32.0))), 8.0, 32.0),
        "score_offset_term": jnp.clip(jax.random.uniform(seeds[7], (1,), jnp.float32, -8.0, -3.0), -8.0, -3.0),
    }


def layer_norm(values, norm_gain):
    average = lax.optimization_barrier(jnp.mean(values, axis=-1, keepdims=True))
    centred = values - average
    spread = lax.optimization_barrier(jnp.mean(centred * centred, axis=-1, keepdims=True))
    return centred * lax.rsqrt(spread + 1e-06) * norm_gain

def unit_vector(vector):
    length = jnp.sqrt(lax.optimization_barrier(jnp.sum(vector * vector, axis=-1, keepdims=True)))
    return (vector / jnp.maximum(length, 1.0)).astype(jnp.bfloat16)

def blocked_sum(image_units, contracting_matrix):
    quarter_width = MLP // N_MP
    running_sum = jnp.zeros((image_units.shape[0], contracting_matrix.shape[1]), jnp.float32)
    for quarter in range(N_MP):
        quarter_sum = jnp.dot(image_units[:, quarter * quarter_width:(quarter + 1) * quarter_width], contracting_matrix[quarter * quarter_width:(quarter + 1) * quarter_width, :], preferred_element_type=jnp.float32)
        rounded = lax.optimization_barrier(quarter_sum.astype(jnp.bfloat16))
        running_sum = running_sum + rounded.astype(jnp.float32)
    return running_sum

def reference(picture_skip_activations, caption_closing_activations, normaliser_multipliers, widening_matrix, contracting_matrix, caption_mapping_matrix, sharpness_factor, score_offset_term):

    def image_block(image_rows):
        as_float = image_rows.astype(jnp.float32)
        image_normed = layer_norm(as_float, normaliser_multipliers[0]).astype(jnp.bfloat16)
        image_units = jax.nn.gelu(jnp.dot(image_normed, widening_matrix, preferred_element_type=jnp.float32), approximate=True).astype(jnp.bfloat16)
        image_final = layer_norm(as_float + blocked_sum(image_units, contracting_matrix), normaliser_multipliers[1])
        return lax.optimization_barrier(jnp.mean(image_final.reshape(IMG_DEV, PATCHES, D), axis=1))
    grouped = picture_skip_activations.reshape(N_DP, IMG_DEV * PATCHES, D)
    image_pooled = lax.map(image_block, grouped).reshape(PAIRS, D)
    picture_code_direction = unit_vector(image_pooled)
    text_normed = layer_norm(caption_closing_activations.astype(jnp.float32), normaliser_multipliers[2]).astype(jnp.bfloat16)
    text_vector = jnp.dot(text_normed, caption_mapping_matrix, preferred_element_type=jnp.float32)
    caption_code_direction = unit_vector(text_vector)
    matching_scores = sharpness_factor[0] * jnp.dot(picture_code_direction, caption_code_direction.T, preferred_element_type=jnp.float32) + score_offset_term[0]
    labels = 2.0 * jnp.eye(PAIRS, dtype=jnp.float32) - 1.0
    loss_terms = jax.nn.softplus(-labels * matching_scores)
    return (lax.optimization_barrier(jnp.sum(loss_terms, axis=1)), lax.optimization_barrier(jnp.sum(loss_terms, axis=0)))
```

```python
import jax
import jax.numpy as jnp
from jax import lax
from jax.experimental import pallas as pl
from jax.experimental.pallas import tpu as pltpu
from jax.sharding import Mesh
from jax.sharding import PartitionSpec as P

D = 1152
HID = 1152
PATCHES = 256
PAIRS = 512
DP = ("y", "xh", "z")
XS = ("xh", "xl")
ALL = ("y", "xh", "z", "xl", "c")
OFFS = (0, -1, 1, 2)
W1A, W1B, W2A, W2B, TX = 80, 64, 64, 80, 16
BF = jnp.bfloat16
F32 = jnp.float32


def shifted(array, axes, by):
    return lax.ppermute(array, axes, [(i, (i + by) % 4) for i in range(4)])


def ring_of_4(first, second, axes):
    right = (shifted(first, axes, 1), shifted(second, axes, 1))
    left = (shifted(first, axes, -1), shifted(second, axes, -1))
    far_first = shifted(right[0], axes, 1)
    far_second = shifted(left[1], axes, -1)
    return (first, right[0], left[0], far_first), (second, right[1], left[1], far_second)


def layer_norm(values, norm_gain):
    average = jnp.mean(values, axis=-1, keepdims=True)
    centred = values - average
    spread = jnp.mean(centred * centred, axis=-1, keepdims=True)
    return centred * lax.rsqrt(spread + 1e-06) * norm_gain


def place():
    x = lax.axis_index("xh") * 2 + lax.axis_index("xl")
    return x, lax.axis_index("y")


def copies(a_refs, b_refs, a_rows, b_rows, dst, sems):
    x, y = place()
    started = []
    for j in range(4):
        for i in range(4):
            for refs, rows, first, xo, yo in (
                (a_refs, a_rows, 0, OFFS[i], OFFS[j]),
                (b_refs, b_rows, a_rows, OFFS[j], OFFS[i]),
            ):
                xx = lax.rem(x + xo + 4, 4)
                yy = lax.rem(y + yo + 4, 4)
                at = pl.multiple_of((yy * 2 + xx // 2) * 144 + first, 16)
                copy = pltpu.make_async_copy(
                    refs[j].at[i, pl.ds(0, rows), :],
                    dst.at[lax.rem(xx, 2), pl.ds(at, rows), :],
                    sems.at[len(started)],
                )
                copy.start()
                started.append(copy)
    for copy in started:
        copy.wait()


def first_kernel(normed_ref, *refs):
    a_refs, b_refs, (h_ref, dst, sems) = refs[:4], refs[4:8], refs[8:]
    copies(a_refs, b_refs, W1A, W1B, dst, sems)
    for r in range(4):
        rows = pl.ds(r * 256, 256)
        for k in range(2):
            v = jnp.dot(normed_ref[rows, :], dst[k], preferred_element_type=F32)
            inner = 0.7978845608028654 * (v + 0.044715 * (v * v * v))
            h_ref[rows, pl.ds(k * HID, HID)] = (0.5 * v * (1.0 + jnp.tanh(inner))).astype(BF)


def second_kernel(own, h_ref, *refs):
    a_refs, b_refs, (out_ref, dst, sems) = refs[:4], refs[4:8], refs[8:]
    copies(a_refs, b_refs, W2A, W2B, dst, sems)
    core = lax.axis_index("c")
    half = core if own else 1 - core
    for r in range(2):
        rows = pl.ds(pl.multiple_of(half * 512 + r * 256, 256), 256)
        total = None
        for k in range(2):
            part = lax.dot_general(
                h_ref[rows, pl.ds(k * HID, HID)],
                dst[k],
                (((1,), (1,)), ((), ())),
                preferred_element_type=F32,
            )
            total = part if total is None else total + part
        out_ref[pl.ds(r * 256, 256), :] = total.astype(out_ref.dtype)


def text_kernel(gain_ref, map_ref, *refs):
    a_refs, b_refs, (out_ref, dst, sems) = refs[:4], refs[4:8], refs[8:]
    x, y = place()
    started = []
    for j in range(4):
        for i in range(4):
            for refs_, first, half, xo, yo in (
                (a_refs, W1A, 0, OFFS[i], OFFS[j]),
                (b_refs, W1B, 1, OFFS[j], OFFS[i]),
            ):
                xx = lax.rem(x + xo + 4, 4)
                yy = lax.rem(y + yo + 4, 4)
                at = pl.multiple_of((yy * 4 + xx) * 32 + half * 16, 16)
                copy = pltpu.make_async_copy(
                    refs_[j].at[i, pl.ds(first, TX), :], dst.at[pl.ds(at, TX), :], sems.at[len(started)]
                )
                copy.start()
                started.append(copy)
    for copy in started:
        copy.wait()
    normed = layer_norm(dst[...].astype(F32), gain_ref[...]).astype(BF)
    vector = jnp.dot(normed, map_ref[...], preferred_element_type=F32)
    length = jnp.sqrt(jnp.sum(vector * vector, axis=-1, keepdims=True))
    out_ref[...] = (vector / jnp.maximum(length, 1.0)).astype(BF)


def last_kernel(scale_ref, shift_ref, x_ref, own_ref, recv_ref, gain_ref, text_ref, cols_ref, rows_ref):
    pooled = []
    for k in range(2):
        rows = pl.ds(k * PATCHES, PATCHES)
        v = x_ref[rows, :].astype(F32) + (own_ref[rows, :] + recv_ref[rows, :].astype(F32))
        final = layer_norm(v, gain_ref[...])
        pooled.append(jnp.mean(final, axis=0, keepdims=True))
    vector = jnp.concatenate(pooled + [jnp.zeros((6, D), F32)], axis=0)
    length = jnp.sqrt(jnp.sum(vector * vector, axis=-1, keepdims=True))
    emb = (vector / jnp.maximum(length, 1.0)).astype(BF)
    scores = (
        lax.dot_general(emb, text_ref[...], (((1,), (1,)), ((), ())), preferred_element_type=F32)
        * scale_ref[0]
        + shift_ref[0]
    )
    dp = lax.axis_index("y") * 16 + lax.axis_index("xh") * 8 + lax.axis_index("z")
    image = dp * 8 + lax.axis_index("xl") * 4 + lax.axis_index("c") * 2
    row = lax.broadcasted_iota(jnp.int32, (8, PAIRS), 0)
    col = lax.broadcasted_iota(jnp.int32, (8, PAIRS), 1)
    t, z, xl, dp_hi = col % 4, (col // 4) % 8, (col // 32) % 2, col // 64
    text = dp_hi * 64 + z * 8 + xl * 4 + t
    value = jnp.where(text == image + row, -scores, scores)
    terms = jnp.maximum(value, 0.0) + jnp.log1p(jnp.exp(-jnp.abs(value)))
    terms = jnp.where(row < 2, terms, 0.0)
    cols_ref[...] = jnp.sum(terms, axis=0, keepdims=True)
    rows_ref[...] = jnp.broadcast_to(jnp.sum(terms, axis=1, keepdims=True), (8, 128))


ANY = pl.BlockSpec(memory_space=pl.ANY)
VM = pl.BlockSpec(memory_space=pltpu.VMEM)
SM = pl.BlockSpec(memory_space=pltpu.SMEM)


def gathered_call(kernel, first, pieces, out, dst, name):
    return pl.pallas_call(
        kernel,
        out_shape=out,
        in_specs=[VM] * len(first) + [ANY] * 8,
        out_specs=VM,
        scratch_shapes=[pltpu.VMEM(dst, BF), pltpu.SemaphoreType.DMA((32,))],
        name=name,
    )(*first, *pieces)


def on_device(
    picture_skip_activations,
    caption_closing_activations,
    normaliser_multipliers,
    widening_matrix,
    contracting_matrix,
    caption_mapping_matrix,
    sharpness_factor,
    score_offset_term,
):
    xl, core = lax.axis_index("xl"), lax.axis_index("c")
    texts = lax.dynamic_slice_in_dim(caption_closing_activations, xl * 4, 4, 0)
    weights = jnp.concatenate([widening_matrix, contracting_matrix.T], axis=0)
    weights = jnp.pad(weights, ((0, 0), (0, HID - weights.shape[1])))
    shard = jnp.concatenate([weights, texts], axis=0)
    along_z = lax.all_to_all(jnp.broadcast_to(shard[None], (8, *shard.shape)), "z", 0, 0, tiled=True)
    w1 = along_z[:, :18].reshape(144, HID)
    w2 = along_z[:, 18:36].reshape(144, HID)
    tx = along_z[:, 36:].reshape(32, D)
    a1 = jnp.concatenate([w1[:W1A], tx[:TX]], axis=0)
    b1 = jnp.concatenate([w1[W1A:], tx[TX:]], axis=0)
    a2, b2 = w2[:W2A], w2[W2A:]

    ax1, ax2 = ring_of_4(a1, a2, XS)
    by1, by2 = ring_of_4(b1, b2, "y")
    ay1, ay2 = ring_of_4(jnp.stack(ax1), jnp.stack(ax2), "y")
    bx1, bx2 = ring_of_4(jnp.stack(by1), jnp.stack(by2), XS)

    image_rows = lax.dynamic_slice_in_dim(picture_skip_activations, xl * 1024, 1024, 0)
    normed = layer_norm(image_rows.astype(F32), normaliser_multipliers[0]).astype(BF)
    own_rows = lax.dynamic_slice_in_dim(picture_skip_activations, xl * 1024 + core * 512, 512, 0)

    pieces1, pieces2 = (*ay1, *bx1), (*ay2, *bx2)
    weight_dst = (2, D, HID)
    units = gathered_call(
        first_kernel, (normed,), pieces1, jax.ShapeDtypeStruct((1024, 2 * HID), BF), weight_dst, "widen"
    )
    text_emb = gathered_call(
        text_kernel,
        (normaliser_multipliers[2:3], caption_mapping_matrix),
        pieces1,
        jax.ShapeDtypeStruct((PAIRS, D), BF),
        (PAIRS, D),
        "text",
    )
    sent = gathered_call(
        lambda *refs: second_kernel(False, *refs),
        (units,),
        pieces2,
        jax.ShapeDtypeStruct((512, D), BF),
        weight_dst,
        "contract_sent",
    )
    received = lax.ppermute(sent, "c", [(0, 1), (1, 0)])
    own = gathered_call(
        lambda *refs: second_kernel(True, *refs),
        (units,),
        pieces2,
        jax.ShapeDtypeStruct((512, D), F32),
        weight_dst,
        "contract_own",
    )
    cols, rows = pl.pallas_call(
        last_kernel,
        out_shape=(jax.ShapeDtypeStruct((1, PAIRS), F32), jax.ShapeDtypeStruct((8, 128), F32)),
        in_specs=[SM, SM, VM, VM, VM, VM, VM],
        out_specs=(VM, VM),
        name="losses",
    )(sharpness_factor, score_offset_term, own_rows, own, received, normaliser_multipliers[1:2], text_emb)

    dp = lax.axis_index(DP)
    cols = cols.reshape(8, 2, 8, 4).transpose(0, 2, 1, 3).reshape(64, 1, 8)
    slot = lax.broadcasted_iota(jnp.int32, (64, 1, 8), 2) - (xl * 4 + core * 2)
    mine = lax.broadcasted_iota(jnp.int32, (64, 1, 8), 0) == dp
    row_part = jnp.where(
        mine & (slot == 0), rows[0, 0], jnp.where(mine & (slot == 1), rows[1, 0], 0.0)
    )
    message = jnp.concatenate([cols, row_part], axis=2)
    message = jnp.broadcast_to(message, (64, 4, 16)).reshape(256, 16)
    arrived = jnp.sum(lax.all_to_all(message, ALL, 0, 0, tiled=True), axis=0)
    return arrived[8:], arrived[:8]


def solution(mesh):
    finer = Mesh(mesh.devices.reshape(4, 2, 8, 2, 2), ALL)
    dp, mp = DP, ("xl", "c")
    in_specs = (P(dp, None), P(dp, None), P(), P(dp, mp), P(mp, dp), P(), P(), P())
    out_specs = (P(dp), P(dp))
    return jax.shard_map(
        on_device, mesh=finer, in_specs=in_specs, out_specs=out_specs, check_vma=False
    )
```

```python
import jax
import jax.numpy as jnp
from jax import lax
from jax.experimental import pallas as pl
from jax.experimental.pallas import tpu as pltpu
from jax.sharding import Mesh
from jax.sharding import PartitionSpec as P

D = 1152
HID = 1152
PATCHES = 256
PAIRS = 512
DP = ("y", "xh", "z")
XS = ("xh", "xl")
ALL = ("y", "xh", "z", "xl", "c")
OFFS = (0, -1, 1, 2)
W1A, W1B, W2A, W2B, TX = 80, 64, 64, 80, 16
BF = jnp.bfloat16
F32 = jnp.float32


def shifted(array, axes, by, size=4):
    return lax.ppermute(array, axes, [(i, (i + by) % size) for i in range(size)])


def ring_whole(block, axes):
    right, left = shifted(block, axes, 1), shifted(block, axes, -1)
    return block, right, left, shifted(right, axes, 1)


def ring_of_4(first, second, axes):
    right1, left1 = shifted(first, axes, 1), shifted(first, axes, -1)
    right2, left2 = shifted(second, axes, 1), shifted(second, axes, -1)
    far1, far2 = shifted(right1, axes, 1), shifted(left2, axes, -1)
    return (first, right1, left1, far1), (second, right2, left2, far2)


def gathered_along_z(block):
    one_r, one_l = shifted(block, "z", 1, 8), shifted(block, "z", -1, 8)
    two_r, two_l = shifted(block, "z", 2, 8), shifted(block, "z", -2, 8)
    three_r, three_l = shifted(two_r, "z", 1, 8), shifted(two_l, "z", -1, 8)
    four = shifted(two_r, "z", 2, 8)
    z = lax.axis_index("z")
    out = jnp.zeros((8, *block.shape), block.dtype)
    pieces = ((0, block), (-1, one_r), (1, one_l), (-2, two_r), (2, two_l), (-3, three_r), (3, three_l), (4, four))
    for by, piece in pieces:
        out = lax.dynamic_update_slice(out, piece[None], (lax.rem(z + by + 8, 8), 0, 0))
    return out


def layer_norm(values, norm_gain):
    average = jnp.mean(values, axis=-1, keepdims=True)
    centred = values - average
    spread = jnp.mean(centred * centred, axis=-1, keepdims=True)
    return centred * lax.rsqrt(spread + 1e-06) * norm_gain


def place():
    x = lax.axis_index("xh") * 2 + lax.axis_index("xl")
    return x, lax.axis_index("y")


def start_copies(a_refs, b_refs, a_rows, b_rows, dst, sems):
    x, y = place()
    groups = ([], [])
    n = 0
    for j in range(4):
        for i in range(4):
            for refs, rows, first, xk, yk in ((a_refs, a_rows, 0, i, j), (b_refs, b_rows, a_rows, j, i)):
                xx = lax.rem(x + OFFS[xk] + 4, 4)
                yy = lax.rem(y + OFFS[yk] + 4, 4)
                at = pl.multiple_of((yy * 2 + xx // 2) * 144 + first, 16)
                copy = pltpu.make_async_copy(
                    refs[j].at[i, pl.ds(0, rows), :],
                    dst.at[lax.rem(xx, 2), pl.ds(at, rows), :],
                    sems.at[n],
                )
                copy.start()
                n += 1
                groups[0 if xk in (0, 3) else 1].append(copy)
    return groups


ROWS = 512


def gelu(v):
    inner = 0.7978845608028654 * (v + 0.044715 * (v * v * v))
    return (0.5 * v * (1.0 + jnp.tanh(inner))).astype(BF)


def block_kernel(normed_ref, *refs):
    first, second, (sent_ref, own_ref, w1, w2, h, sems1, sems2) = refs[:8], refs[8:16], refs[16:]
    copies1 = start_copies(first[:4], first[4:], W1A, W1B, w1, sems1)
    copies2 = start_copies(second[:4], second[4:], W2A, W2B, w2, sems2)
    near = lax.rem(lax.axis_index("xl"), 2)
    core = lax.axis_index("c")
    for copy in copies1[0]:
        copy.wait()

    def widen(t, _):
        @pl.when(t == 2)
        def _():
            for copy in copies1[1]:
                copy.wait()

        k = lax.rem(near + t // 2, 2)
        rows = pl.ds(pl.multiple_of(lax.rem(t, 2) * ROWS, ROWS), ROWS)
        h[k, rows, :] = gelu(jnp.dot(normed_ref[rows, :], w1[k], preferred_element_type=F32))
        return 0

    lax.fori_loop(0, 4, widen, 0)
    for group in range(2):
        for copy in copies2[group]:
            copy.wait()

    def contract(t, _):
        half = lax.rem(core + 1 + t, 2)
        rows = pl.ds(pl.multiple_of(half * ROWS, ROWS), ROWS)
        total = None
        for k in range(2):
            part = lax.dot_general(
                h[k, rows, :], w2[k], (((1,), (1,)), ((), ())), preferred_element_type=F32
            )
            total = part if total is None else total + part
        own_ref[...] = total

        @pl.when(t == 0)
        def _():
            sent_ref[...] = own_ref[...].astype(BF)

        return 0

    lax.fori_loop(0, 2, contract, 0)


def text_kernel(gain_ref, map_ref, *refs):
    a_refs, b_refs, (out_ref, dst, sems) = refs[:4], refs[4:8], refs[8:]
    x, y = place()
    started = []
    for j in range(4):
        for i in range(4):
            for refs_, first, half, xo, yo in (
                (a_refs, W1A, 0, OFFS[i], OFFS[j]),
                (b_refs, W1B, 1, OFFS[j], OFFS[i]),
            ):
                xx = lax.rem(x + xo + 4, 4)
                yy = lax.rem(y + yo + 4, 4)
                at = pl.multiple_of((yy * 4 + xx) * 32 + half * 16, 16)
                copy = pltpu.make_async_copy(
                    refs_[j].at[i, pl.ds(first, TX), :], dst.at[pl.ds(at, TX), :], sems.at[len(started)]
                )
                copy.start()
                started.append(copy)
    for copy in started:
        copy.wait()
    normed = layer_norm(dst[...].astype(F32), gain_ref[...]).astype(BF)
    vector = jnp.dot(normed, map_ref[...], preferred_element_type=F32)
    length = jnp.sqrt(jnp.sum(vector * vector, axis=-1, keepdims=True))
    out_ref[...] = (vector / jnp.maximum(length, 1.0)).astype(BF)


def last_kernel(scale_ref, shift_ref, x_ref, own_ref, recv_ref, gain_ref, text_ref, out_ref):
    pooled = []
    for k in range(2):
        rows = pl.ds(k * PATCHES, PATCHES)
        v = x_ref[rows, :].astype(F32) + (own_ref[rows, :] + recv_ref[rows, :].astype(F32))
        final = layer_norm(v, gain_ref[...])
        pooled.append(jnp.mean(final, axis=0, keepdims=True))
    vector = jnp.concatenate(pooled + [jnp.zeros((6, D), F32)], axis=0)
    length = jnp.sqrt(jnp.sum(vector * vector, axis=-1, keepdims=True))
    emb = (vector / jnp.maximum(length, 1.0)).astype(BF)
    scores = (
        lax.dot_general(text_ref[...], emb, (((1,), (1,)), ((), ())), preferred_element_type=F32)
        * scale_ref[0]
        + shift_ref[0]
    )
    dp = lax.axis_index("y") * 16 + lax.axis_index("xh") * 8 + lax.axis_index("z")
    slot = lax.axis_index("xl") * 4 + lax.axis_index("c") * 2
    q = lax.broadcasted_iota(jnp.int32, (PAIRS, 8), 0)
    col = lax.broadcasted_iota(jnp.int32, (PAIRS, 8), 1)
    q_dp, q_slot = (q // 64) * 8 + (q // 4) % 8, ((q // 32) % 2) * 4 + q % 4
    own_pair = (q_dp == dp) & (q_slot == slot + col)
    value = jnp.where(own_pair, -scores, scores)
    terms = jnp.maximum(value, 0.0) + jnp.log1p(jnp.exp(-jnp.abs(value)))
    terms = jnp.where(col < 2, terms, 0.0)
    cols = jnp.sum(terms, axis=1, keepdims=True)
    rows = jnp.sum(terms, axis=0, keepdims=True)
    spread = jnp.where(q_slot == col, cols, 0.0)
    r = lax.broadcasted_iota(jnp.int32, (64, PAIRS), 0)
    c = lax.broadcasted_iota(jnp.int32, (64, PAIRS), 1)
    owner = jnp.where((c // 64) * 8 + (c // 4) % 8 == r, 1.0, 0.0)
    col_part = jnp.dot(owner, spread, precision=lax.Precision.HIGHEST, preferred_element_type=F32)
    mr = lax.broadcasted_iota(jnp.int32, (64, 8), 0)
    mc = lax.broadcasted_iota(jnp.int32, (64, 8), 1)
    row_part = jnp.where(mc == slot, rows[:, 0:1], jnp.where(mc == slot + 1, rows[:, 1:2], 0.0))
    row_part = jnp.where(mr == dp, row_part, 0.0)
    message = jnp.concatenate([col_part, row_part], axis=1)
    for m in range(4):
        out_ref[:, m, :] = message


ANY = pl.BlockSpec(memory_space=pl.ANY)
VM = pl.BlockSpec(memory_space=pltpu.VMEM)
SM = pl.BlockSpec(memory_space=pltpu.SMEM)


def on_device(
    picture_skip_activations,
    caption_closing_activations,
    normaliser_multipliers,
    widening_matrix,
    contracting_matrix,
    caption_mapping_matrix,
    sharpness_factor,
    score_offset_term,
):
    xl, core = lax.axis_index("xl"), lax.axis_index("c")
    texts = lax.dynamic_slice_in_dim(caption_closing_activations, xl * 4, 4, 0)
    weights = jnp.concatenate([widening_matrix, contracting_matrix.T], axis=0)
    weights = jnp.pad(weights, ((0, 0), (0, HID - weights.shape[1])))
    shard = jnp.concatenate([weights, texts], axis=0)
    along_z = gathered_along_z(shard)
    w1 = along_z[:, :18].reshape(144, HID)
    w2 = along_z[:, 18:36].reshape(144, HID)
    tx = along_z[:, 36:].reshape(32, D)
    a = jnp.concatenate([w1[:W1A], tx[:TX], w2[:W2A]], axis=0)
    b = jnp.concatenate([w1[W1A:], tx[TX:], w2[W2A:]], axis=0)

    a, b = jnp.stack(ring_whole(a, XS)), jnp.stack(ring_whole(b, "y"))
    ay1, ay2 = ring_of_4(a[:, : W1A + TX], a[:, W1A + TX :], "y")
    bx1, bx2 = ring_of_4(b[:, : W1B + TX], b[:, W1B + TX :], XS)

    image_rows = lax.dynamic_slice_in_dim(picture_skip_activations, xl * 1024, 1024, 0)
    own_rows = lax.dynamic_slice_in_dim(picture_skip_activations, xl * 1024 + core * 512, 512, 0)
    normed = layer_norm(image_rows.astype(F32), normaliser_multipliers[0]).astype(BF)

    pieces1, pieces2 = (*ay1, *bx1), (*ay2, *bx2)
    sent, own = pl.pallas_call(
        block_kernel,
        out_shape=(jax.ShapeDtypeStruct((512, D), BF), jax.ShapeDtypeStruct((512, D), F32)),
        in_specs=[VM] + [ANY] * 16,
        out_specs=(VM, VM),
        scratch_shapes=[
            pltpu.VMEM((2, D, HID), BF),
            pltpu.VMEM((2, D, HID), BF),
            pltpu.VMEM((2, 1024, HID), BF),
            pltpu.SemaphoreType.DMA((32,)),
            pltpu.SemaphoreType.DMA((32,)),
        ],
        name="block",
        compiler_params=pltpu.CompilerParams(vmem_limit_bytes=36 << 20),
    )(normed, *pieces1, *pieces2)
    received = lax.ppermute(sent, "c", [(0, 1), (1, 0)])
    text_emb = pl.pallas_call(
        text_kernel,
        out_shape=jax.ShapeDtypeStruct((PAIRS, D), BF),
        in_specs=[VM, VM] + [ANY] * 8,
        out_specs=VM,
        scratch_shapes=[pltpu.VMEM((PAIRS, D), BF), pltpu.SemaphoreType.DMA((32,))],
        name="text",
        compiler_params=pltpu.CompilerParams(vmem_limit_bytes=24 << 20),
    )(normaliser_multipliers[2:3], caption_mapping_matrix, *pieces1)
    message = pl.pallas_call(
        last_kernel,
        out_shape=jax.ShapeDtypeStruct((64, 4, 16), F32),
        in_specs=[SM, SM, VM, VM, VM, VM, VM],
        out_specs=VM,
        name="losses",
        compiler_params=pltpu.CompilerParams(vmem_limit_bytes=24 << 20),
    )(sharpness_factor, score_offset_term, own_rows, own, received, normaliser_multipliers[1:2], text_emb)
    arrived = jnp.sum(lax.all_to_all(message.reshape(256, 16), ALL, 0, 0, tiled=True), axis=0)
    return arrived[8:], arrived[:8]


def solution(mesh):
    finer = Mesh(mesh.devices.reshape(4, 2, 8, 2, 2), ALL)
    dp, mp = DP, ("xl", "c")
    in_specs = (P(dp, None), P(dp, None), P(), P(dp, mp), P(mp, dp), P(), P(), P())
    out_specs = (P(dp), P(dp))
    return jax.shard_map(
        on_device, mesh=finer, in_specs=in_specs, out_specs=out_specs, check_vma=False
    )
```

```python
import jax
import jax.numpy as jnp
from jax import lax
from jax.experimental import pallas as pl
from jax.experimental.pallas import tpu as pltpu
from jax.sharding import Mesh
from jax.sharding import PartitionSpec as P

D = 1152
HID = 1152
PATCHES = 256
PAIRS = 512
DP = ("y", "xh", "z")
XS = ("xh", "xl")
ALL = ("y", "xh", "z", "xl", "c")
W1A, W1B, W2A, W2B, TX = 80, 64, 64, 80, 16
BF = jnp.bfloat16
F32 = jnp.float32


def shifted(array, axes, by, size=4):
    return lax.ppermute(array, axes, [(i, (i + by) % size) for i in range(size)])


def small_ring(block, cut, axes):
    right, left = shifted(block, axes, 1), shifted(block, axes, -1)
    far1, far2 = shifted(right[:cut], axes, 1), shifted(left[cut:], axes, -1)
    first = jnp.stack([block[:cut], right[:cut], far1, left[:cut]])
    return first, jnp.stack([block[cut:], right[cut:], far2, left[cut:]])


def large_ring(block, axes):
    right, left = shifted(block, axes, 1), shifted(block, axes, -1)
    return block, right, left, shifted(right[:2], axes, 1), shifted(left[2:], axes, -1)


def after(block, ring):
    return lax.optimization_barrier((block, ring[1], ring[2]))[0]


def gathered_along_z(block):
    one_r, one_l = shifted(block, "z", 1, 8), shifted(block, "z", -1, 8)
    two_r, two_l = shifted(block, "z", 2, 8), shifted(block, "z", -2, 8)
    three_r, three_l = shifted(two_r, "z", 1, 8), shifted(two_l, "z", -1, 8)
    four = shifted(two_r, "z", 2, 8)
    z = lax.axis_index("z")
    out = jnp.zeros((8, *block.shape), block.dtype)
    pieces = ((0, block), (-1, one_r), (1, one_l), (-2, two_r), (2, two_l), (-3, three_r), (3, three_l), (4, four))
    for by, piece in pieces:
        out = lax.dynamic_update_slice(out, piece[None], (lax.rem(z + by + 8, 8), 0, 0))
    return out


def layer_norm(values, norm_gain):
    average = jnp.mean(values, axis=-1, keepdims=True)
    centred = values - average
    spread = jnp.mean(centred * centred, axis=-1, keepdims=True)
    return centred * lax.rsqrt(spread + 1e-06) * norm_gain


def place():
    x = lax.axis_index("xh") * 2 + lax.axis_index("xl")
    return x, lax.axis_index("y")


def each_piece(a_refs, b_refs, write):
    x, y = place()

    def visit(ref, n, i, j, half):
        xk, yk = (i, j) if half == 0 else (j, i)
        write(half, ref, n, lax.rem(x - xk + 4, 4), lax.rem(y - yk + 4, 4))

    def whole(i, _):
        for half, refs in enumerate((a_refs, b_refs)):
            for ref, j in ((refs[0], 0), (refs[1], 1), (refs[2], 3)):
                visit(ref, i, i, j, half)
        return 0

    def halves(u, _):
        for half, refs in enumerate((a_refs, b_refs)):
            visit(refs[3], u, u, 2, half)
            visit(refs[4], u, u + 2, 2, half)
        return 0

    lax.fori_loop(0, 4, whole, 0)
    lax.fori_loop(0, 2, halves, 0)


def put_in_order(rows, dst, ref, half, n, xx, yy):
    at = pl.multiple_of((yy * 2 + xx // 2) * 144 + half * rows[0], 16)
    dst[lax.rem(xx, 2), pl.ds(at, rows[half]), :] = ref[n, 0 : rows[half], :]


ROWS = 512


def gelu(v):
    inner = 0.7978845608028654 * (v + 0.044715 * (v * v * v))
    return (0.5 * v * (1.0 + jnp.tanh(inner))).astype(BF)


def norm_kernel(x_ref, gain_ref, normed_ref, own_ref, sem):
    first = pl.multiple_of(lax.axis_index("xl") * 1024, 1024)
    copy = pltpu.make_async_copy(x_ref.at[pl.ds(first, 1024), :], normed_ref, sem)
    copy.start()
    copy.wait()
    half = pl.multiple_of(lax.axis_index("c") * 512, 512)
    gain = gain_ref[...]

    def keep(r, _):
        rows = pl.multiple_of(r * 64, 64)
        own_ref[pl.ds(rows, 64), :] = normed_ref[pl.ds(half + rows, 64), :]
        return 0

    def norm(r, _):
        rows = pl.ds(pl.multiple_of(r * 32, 32), 32)
        normed_ref[rows, :] = layer_norm(normed_ref[rows, :].astype(F32), gain).astype(BF)
        return 0

    lax.fori_loop(0, 8, keep, 0)
    lax.fori_loop(0, 32, norm, 0)


def widen_kernel(normed_ref, *refs):
    a_refs, b_refs, (h, texts, w1) = refs[:5], refs[5:10], refs[10:]
    rows = (W1A, W1B)

    def write(half, ref, n, xx, yy):
        put_in_order(rows, w1, ref, half, n, xx, yy)
        at = pl.multiple_of((yy * 4 + xx) * 32 + half * TX, 16)
        texts[pl.ds(at, TX), :] = ref[n, rows[half] : rows[half] + TX, :]

    each_piece(a_refs, b_refs, write)

    def widen(t, _):
        k = t // 2
        rows = pl.ds(pl.multiple_of(lax.rem(t, 2) * ROWS, ROWS), ROWS)
        h[k, rows, :] = gelu(jnp.dot(normed_ref[rows, :], w1[k], preferred_element_type=F32))
        return 0

    lax.fori_loop(0, 4, widen, 0)


def contract_kernel(h, *refs):
    a_refs, b_refs, (sent_ref, own_ref, w2) = refs[:5], refs[5:10], refs[10:]

    def write(half, ref, n, xx, yy):
        put_in_order((W2A, W2B), w2, ref, half, n, xx, yy)

    each_piece(a_refs, b_refs, write)
    core = lax.axis_index("c")

    def contract(t, _):
        half = lax.rem(core + 1 + t, 2)
        rows = pl.ds(pl.multiple_of(half * ROWS, ROWS), ROWS)
        total = None
        for k in range(2):
            part = lax.dot_general(
                h[k, rows, :], w2[k], (((1,), (1,)), ((), ())), preferred_element_type=F32
            )
            total = part if total is None else total + part
        own_ref[...] = total

        @pl.when(t == 0)
        def _():
            sent_ref[...] = own_ref[...].astype(BF)

        return 0

    lax.fori_loop(0, 2, contract, 0)


def text_kernel(gain_ref, map_ref, rows_ref, out_ref):
    gain = gain_ref[...]

    def embed(r, _):
        rows = pl.ds(pl.multiple_of(r * 256, 256), 256)
        normed = layer_norm(rows_ref[rows, :].astype(F32), gain).astype(BF)
        vector = jnp.dot(normed, map_ref[...], preferred_element_type=F32)
        length = jnp.sqrt(jnp.sum(vector * vector, axis=-1, keepdims=True))
        out_ref[rows, :] = (vector / jnp.maximum(length, 1.0)).astype(BF)
        return 0

    lax.fori_loop(0, PAIRS // 256, embed, 0)


def last_kernel(scale_ref, shift_ref, x_ref, own_ref, recv_ref, gain_ref, text_ref, out_ref):
    gain = gain_ref[...]
    pooled = []
    for k in range(2):

        def pool(r, total, k=k):
            rows = pl.ds(pl.multiple_of(k * PATCHES + r * 64, 64), 64)
            v = x_ref[rows, :].astype(F32) + (own_ref[rows, :] + recv_ref[rows, :].astype(F32))
            final = layer_norm(v, gain)
            return total + jnp.sum(final.reshape(8, 8, D), axis=0)

        total = lax.fori_loop(0, PATCHES // 64, pool, jnp.zeros((8, D), F32))
        pooled.append(jnp.sum(total, axis=0, keepdims=True) * (1.0 / PATCHES))
    vector = jnp.concatenate(pooled + [jnp.zeros((6, D), F32)], axis=0)
    length = jnp.sqrt(jnp.sum(vector * vector, axis=-1, keepdims=True))
    emb = (vector / jnp.maximum(length, 1.0)).astype(BF)
    scores = (
        lax.dot_general(text_ref[...], emb, (((1,), (1,)), ((), ())), preferred_element_type=F32)
        * scale_ref[0]
        + shift_ref[0]
    )
    dp = lax.axis_index("y") * 16 + lax.axis_index("xh") * 8 + lax.axis_index("z")
    slot = lax.axis_index("xl") * 4 + lax.axis_index("c") * 2
    q = lax.broadcasted_iota(jnp.int32, (PAIRS, 8), 0)
    col = lax.broadcasted_iota(jnp.int32, (PAIRS, 8), 1)
    q_dp, q_slot = (q // 64) * 8 + (q // 4) % 8, ((q // 32) % 2) * 4 + q % 4
    own_pair = (q_dp == dp) & (q_slot == slot + col)
    value = jnp.where(own_pair, -scores, scores)
    terms = jnp.maximum(value, 0.0) + jnp.log1p(jnp.exp(-jnp.abs(value)))
    terms = jnp.where(col < 2, terms, 0.0)
    cols = jnp.sum(terms, axis=1, keepdims=True)
    rows = jnp.sum(terms, axis=0, keepdims=True)
    spread = jnp.where(q_slot == col, cols, 0.0)
    r = lax.broadcasted_iota(jnp.int32, (64, PAIRS), 0)
    c = lax.broadcasted_iota(jnp.int32, (64, PAIRS), 1)
    owner = jnp.where((c // 64) * 8 + (c // 4) % 8 == r, 1.0, 0.0)
    col_part = jnp.dot(owner, spread, precision=lax.Precision.HIGHEST, preferred_element_type=F32)
    mr = lax.broadcasted_iota(jnp.int32, (64, 8), 0)
    mc = lax.broadcasted_iota(jnp.int32, (64, 8), 1)
    row_part = jnp.where(mc == slot, rows[:, 0:1], jnp.where(mc == slot + 1, rows[:, 1:2], 0.0))
    row_part = jnp.where(mr == dp, row_part, 0.0)
    message = jnp.concatenate([col_part, row_part], axis=1)
    for m in range(4):
        out_ref[:, m, :] = message


ANY = pl.BlockSpec(memory_space=pl.ANY)
VM = pl.BlockSpec(memory_space=pltpu.VMEM)
SM = pl.BlockSpec(memory_space=pltpu.SMEM)


def on_device(
    picture_skip_activations,
    caption_closing_activations,
    normaliser_multipliers,
    widening_matrix,
    contracting_matrix,
    caption_mapping_matrix,
    sharpness_factor,
    score_offset_term,
):
    xl = lax.axis_index("xl")
    texts = lax.dynamic_slice_in_dim(caption_closing_activations, xl * 4, 4, 0)
    weights = jnp.concatenate([widening_matrix, contracting_matrix.T], axis=0)
    weights = jnp.pad(weights, ((0, 0), (0, HID - weights.shape[1])))
    shard = jnp.concatenate([weights, texts], axis=0)
    along_z = gathered_along_z(shard)
    w1 = along_z[:, :18].reshape(144, HID)
    w2 = along_z[:, 18:36].reshape(144, HID)
    tx = along_z[:, 36:].reshape(32, D)
    a = jnp.concatenate([w1[:W1A], tx[:TX], w2[:W2A]], axis=0)
    b = jnp.concatenate([w1[W1A:], tx[TX:], w2[W2A:]], axis=0)

    a1, a2 = small_ring(a, W1A + TX, XS)
    b1, b2 = small_ring(b, W1B + TX, "y")
    a1, b1 = large_ring(a1, "y"), large_ring(b1, XS)
    a2, b2 = large_ring(after(a2, a1), "y"), large_ring(after(b2, b1), XS)

    normed, own_rows = pl.pallas_call(
        norm_kernel,
        out_shape=(jax.ShapeDtypeStruct((1024, D), BF), jax.ShapeDtypeStruct((512, D), BF)),
        in_specs=[ANY, VM],
        out_specs=(VM, VM),
        scratch_shapes=[pltpu.SemaphoreType.DMA],
        name="norm",
        cost_estimate=pl.CostEstimate(flops=20 * 1024 * D, transcendentals=0, bytes_accessed=6 << 20),
        compiler_params=pltpu.CompilerParams(vmem_limit_bytes=8 << 20),
    )(picture_skip_activations, normaliser_multipliers[0:1])

    cost = pl.CostEstimate(flops=4 * 1024 * D * HID, transcendentals=0, bytes_accessed=12 << 20)
    units, texts = pl.pallas_call(
        widen_kernel,
        out_shape=(jax.ShapeDtypeStruct((2, 1024, HID), BF), jax.ShapeDtypeStruct((PAIRS, D), BF)),
        in_specs=[VM] * 11,
        out_specs=(VM, VM),
        scratch_shapes=[pltpu.VMEM((2, D, HID), BF)],
        name="widen",
        cost_estimate=cost,
        compiler_params=pltpu.CompilerParams(vmem_limit_bytes=14 << 20),
    )(normed, *a1, *b1)
    sent, own = pl.pallas_call(
        contract_kernel,
        out_shape=(jax.ShapeDtypeStruct((512, D), BF), jax.ShapeDtypeStruct((512, D), F32)),
        in_specs=[VM] * 11,
        out_specs=(VM, VM),
        scratch_shapes=[pltpu.VMEM((2, D, HID), BF)],
        name="contract",
        cost_estimate=cost,
        compiler_params=pltpu.CompilerParams(vmem_limit_bytes=14 << 20),
    )(units, *a2, *b2)
    received = lax.ppermute(sent, "c", [(0, 1), (1, 0)])
    text_emb = pl.pallas_call(
        text_kernel,
        out_shape=jax.ShapeDtypeStruct((PAIRS, D), BF),
        in_specs=[VM] * 3,
        out_specs=VM,
        name="text",
        cost_estimate=pl.CostEstimate(flops=2 * PAIRS * D * D, transcendentals=0, bytes_accessed=5 << 20),
        compiler_params=pltpu.CompilerParams(vmem_limit_bytes=12 << 20),
    )(normaliser_multipliers[2:3], caption_mapping_matrix, texts)
    message = pl.pallas_call(
        last_kernel,
        out_shape=jax.ShapeDtypeStruct((64, 4, 16), F32),
        in_specs=[SM, SM, VM, VM, VM, VM, VM],
        out_specs=VM,
        name="losses",
        compiler_params=pltpu.CompilerParams(vmem_limit_bytes=12 << 20),
    )(sharpness_factor, score_offset_term, own_rows, own, received, normaliser_multipliers[1:2], text_emb)
    arrived = jnp.sum(lax.all_to_all(message.reshape(256, 16), ALL, 0, 0, tiled=True), axis=0)
    return arrived[8:], arrived[:8]


def solution(mesh):
    finer = Mesh(mesh.devices.reshape(4, 2, 8, 2, 2), ALL)
    dp, mp = DP, ("xl", "c")
    in_specs = (P(dp, None), P(dp, None), P(), P(dp, mp), P(mp, dp), P(), P(), P())
    out_specs = (P(dp), P(dp))
    return jax.shard_map(
        on_device, mesh=finer, in_specs=in_specs, out_specs=out_specs, check_vma=False
    )
```

```python
import jax
import jax.numpy as jnp
from jax import lax
from jax.experimental import pallas as pl
from jax.experimental.pallas import tpu as pltpu
from jax.sharding import Mesh
from jax.sharding import PartitionSpec as P


D = 1152
HID = 1152
PATCHES = 256
PAIRS = 512
DP = ("y", "xh", "z")
XS = ("xh", "xl")
ALL = ("y", "xh", "z", "xl", "c")
W1A, W1B, W2A, W2B, TX = 80, 64, 64, 80, 16
BF = jnp.bfloat16
F32 = jnp.float32


def shifted(array, axes, by, size=4):
    return lax.ppermute(array, axes, [(i, (i + by) % size) for i in range(size)])


def small_ring(block, cut, axes):
    right, left = shifted(block, axes, 1), shifted(block, axes, -1)
    far1, far2 = shifted(right[:cut], axes, 1), shifted(left[cut:], axes, -1)
    first = jnp.stack([block[:cut], right[:cut], far1, left[:cut]])
    return first, jnp.stack([block[cut:], right[cut:], far2, left[cut:]])


def large_ring(block, axes):
    right = shifted(block, axes, 1)
    left = shifted(block, axes, -1)
    far_r = shifted(right[:2], axes, 1)
    far_l = shifted(left[2:], axes, -1)
    return block, right, left, far_r, far_l


def gathered_along_z(block):
    one_r, one_l = shifted(block, "z", 1, 8), shifted(block, "z", -1, 8)
    two_r, two_l = shifted(block, "z", 2, 8), shifted(block, "z", -2, 8)
    three_r, three_l = shifted(two_r, "z", 1, 8), shifted(two_l, "z", -1, 8)
    four = shifted(two_r, "z", 2, 8)
    z = lax.axis_index("z")
    out = jnp.zeros((8, *block.shape), block.dtype)
    pieces = ((0, block), (-1, one_r), (1, one_l), (-2, two_r), (2, two_l), (-3, three_r), (3, three_l), (4, four))
    for by, piece in pieces:
        out = lax.dynamic_update_slice(out, piece[None], (lax.rem(z + by + 8, 8), 0, 0))
    return out


def layer_norm(values, norm_gain):
    average = jnp.mean(values, axis=-1, keepdims=True)
    centred = values - average
    spread = jnp.mean(centred * centred, axis=-1, keepdims=True)
    return centred * lax.rsqrt(spread + 1e-06) * norm_gain


def place():
    x = lax.axis_index("xh") * 2 + lax.axis_index("xl")
    return x, lax.axis_index("y")


def each_piece(a_refs, b_refs, write):
    x, y = place()

    def visit(ref, n, i, j, half):
        xk, yk = (i, j) if half == 0 else (j, i)
        write(half, ref, n, lax.rem(x - xk + 4, 4), lax.rem(y - yk + 4, 4))

    def whole(i, _):
        for half, refs in enumerate((a_refs, b_refs)):
            for ref, j in ((refs[0], 0), (refs[1], 1), (refs[2], 3)):
                visit(ref, i, i, j, half)
        return 0

    def halves(u, _):
        for half, refs in enumerate((a_refs, b_refs)):
            visit(refs[3], u, u, 2, half)
            visit(refs[4], u, u + 2, 2, half)
        return 0

    lax.fori_loop(0, 4, whole, 0)
    lax.fori_loop(0, 2, halves, 0)


def put_in_order(rows, dst, ref, half, n, xx, yy):
    at = pl.multiple_of((yy * 2 + xx // 2) * 144 + half * rows[0], 16)
    dst[lax.rem(xx, 2), pl.ds(at, rows[half]), :] = ref[n, 0 : rows[half], :]


ROWS = 512


def gelu(v):
    inner = 0.7978845608028654 * (v + 0.044715 * (v * v * v))
    return (0.5 * v * (1.0 + jnp.tanh(inner))).astype(BF)


def norm_kernel(x_ref, gain_ref, normed_ref, own_ref, sem):
    first = pl.multiple_of(lax.axis_index("xl") * 1024, 1024)
    copy = pltpu.make_async_copy(x_ref.at[pl.ds(first, 1024), :], normed_ref, sem)
    copy.start()
    copy.wait()
    half = pl.multiple_of(lax.axis_index("c") * 512, 512)
    gain = gain_ref[...]

    def keep(r, _):
        rows = pl.multiple_of(r * 64, 64)
        own_ref[pl.ds(rows, 64), :] = normed_ref[pl.ds(half + rows, 64), :]
        return 0

    def norm(r, _):
        rows = pl.ds(pl.multiple_of(r * 32, 32), 32)
        normed_ref[rows, :] = layer_norm(normed_ref[rows, :].astype(F32), gain).astype(BF)
        return 0

    lax.fori_loop(0, 8, keep, 0)
    lax.fori_loop(0, 32, norm, 0)


def widen_kernel(normed_ref, *refs):
    a_refs, b_refs, (h, texts, w1) = refs[:5], refs[5:10], refs[10:]
    rows = (W1A, W1B)

    def write(half, ref, n, xx, yy):
        put_in_order(rows, w1, ref, half, n, xx, yy)
        at = pl.multiple_of((yy * 4 + xx) * 32 + half * TX, 16)
        texts[pl.ds(at, TX), :] = ref[n, rows[half] : rows[half] + TX, :]

    each_piece(a_refs, b_refs, write)

    def widen(t, _):
        k = t // 2
        rows = pl.ds(pl.multiple_of(lax.rem(t, 2) * ROWS, ROWS), ROWS)
        h[k, rows, :] = gelu(jnp.dot(normed_ref[rows, :], w1[k], preferred_element_type=F32))
        return 0

    lax.fori_loop(0, 4, widen, 0)


def contracted(h, w2, half, out_ref):
    def step(r, _):
        rows = pl.ds(pl.multiple_of(half * 512 + r * 256, 256), 256)
        total = None
        for k in range(2):
            part = lax.dot_general(
                h[k, rows, :], w2[k], (((1,), (1,)), ((), ())), preferred_element_type=F32
            )
            total = part if total is None else total + part
        out_ref[pl.ds(pl.multiple_of(r * 256, 256), 256), :] = total.astype(out_ref.dtype)
        return 0

    lax.fori_loop(0, 2, step, 0)


def contract_sent_kernel(h, *refs):
    a_refs, b_refs, (sent_ref, w2) = refs[:5], refs[5:10], refs[10:]

    def write(half, ref, n, xx, yy):
        put_in_order((W2A, W2B), w2, ref, half, n, xx, yy)

    each_piece(a_refs, b_refs, write)
    contracted(h, w2, 1 - lax.axis_index("c"), sent_ref)


def contract_own_kernel(h, w2, own_ref):
    contracted(h, w2, lax.axis_index("c"), own_ref)


def text_kernel(gain_ref, map_ref, rows_ref, out_ref):
    gain = gain_ref[...]

    def embed(r, _):
        rows = pl.ds(pl.multiple_of(r * 128, 128), 128)
        normed = layer_norm(rows_ref[rows, :].astype(F32), gain).astype(BF)
        vector = jnp.dot(normed, map_ref[...], preferred_element_type=F32)
        length = jnp.sqrt(jnp.sum(vector * vector, axis=-1, keepdims=True))
        out_ref[rows, :] = (vector / jnp.maximum(length, 1.0)).astype(BF)
        return 0

    lax.fori_loop(0, PAIRS // 128, embed, 0)


def last_kernel(scale_ref, shift_ref, x_ref, own_ref, recv_ref, gain_ref, text_ref, out_ref):
    gain = gain_ref[...]
    pooled = []
    for k in range(2):

        def pool(r, total, k=k):
            rows = pl.ds(pl.multiple_of(k * PATCHES + r * 64, 64), 64)
            v = x_ref[rows, :].astype(F32) + (own_ref[rows, :] + recv_ref[rows, :].astype(F32))
            final = layer_norm(v, gain)
            return total + jnp.sum(final.reshape(8, 8, D), axis=0)

        total = lax.fori_loop(0, PATCHES // 64, pool, jnp.zeros((8, D), F32))
        pooled.append(jnp.sum(total, axis=0, keepdims=True) * (1.0 / PATCHES))
    vector = jnp.concatenate(pooled + [jnp.zeros((6, D), F32)], axis=0)
    length = jnp.sqrt(jnp.sum(vector * vector, axis=-1, keepdims=True))
    emb = (vector / jnp.maximum(length, 1.0)).astype(BF)
    scores = (
        lax.dot_general(text_ref[...], emb, (((1,), (1,)), ((), ())), preferred_element_type=F32)
        * scale_ref[0]
        + shift_ref[0]
    )
    dp = lax.axis_index("y") * 16 + lax.axis_index("xh") * 8 + lax.axis_index("z")
    slot = lax.axis_index("xl") * 4 + lax.axis_index("c") * 2
    q = lax.broadcasted_iota(jnp.int32, (PAIRS, 8), 0)
    col = lax.broadcasted_iota(jnp.int32, (PAIRS, 8), 1)
    q_dp, q_slot = (q // 64) * 8 + (q // 4) % 8, ((q // 32) % 2) * 4 + q % 4
    own_pair = (q_dp == dp) & (q_slot == slot + col)
    value = jnp.where(own_pair, -scores, scores)
    terms = jnp.maximum(value, 0.0) + jnp.log1p(jnp.exp(-jnp.abs(value)))
    terms = jnp.where(col < 2, terms, 0.0)
    cols = jnp.sum(terms, axis=1, keepdims=True)
    rows = jnp.sum(terms, axis=0, keepdims=True)
    spread = jnp.where(q_slot == col, cols, 0.0)
    r = lax.broadcasted_iota(jnp.int32, (64, PAIRS), 0)
    c = lax.broadcasted_iota(jnp.int32, (64, PAIRS), 1)
    owner = jnp.where((c // 64) * 8 + (c // 4) % 8 == r, 1.0, 0.0)
    col_part = jnp.dot(owner, spread, precision=lax.Precision.HIGHEST, preferred_element_type=F32)
    mr = lax.broadcasted_iota(jnp.int32, (64, 8), 0)
    mc = lax.broadcasted_iota(jnp.int32, (64, 8), 1)
    row_part = jnp.where(mc == slot, rows[:, 0:1], jnp.where(mc == slot + 1, rows[:, 1:2], 0.0))
    row_part = jnp.where(mr == dp, row_part, 0.0)
    message = jnp.concatenate([col_part, row_part], axis=1)
    for m in range(4):
        out_ref[:, m, :] = message


ANY = pl.BlockSpec(memory_space=pl.ANY)
VM = pl.BlockSpec(memory_space=pltpu.VMEM)
SM = pl.BlockSpec(memory_space=pltpu.SMEM)


def on_device(
    picture_skip_activations,
    caption_closing_activations,
    normaliser_multipliers,
    widening_matrix,
    contracting_matrix,
    caption_mapping_matrix,
    sharpness_factor,
    score_offset_term,
):
    xl = lax.axis_index("xl")
    texts = lax.dynamic_slice_in_dim(caption_closing_activations, xl * 4, 4, 0)
    weights = jnp.concatenate([widening_matrix, contracting_matrix.T], axis=0)
    weights = jnp.pad(weights, ((0, 0), (0, HID - weights.shape[1])))
    shard = jnp.concatenate([weights, texts], axis=0)
    along_z = gathered_along_z(shard)
    w1 = along_z[:, :18].reshape(144, HID)
    w2 = along_z[:, 18:36].reshape(144, HID)
    tx = along_z[:, 36:].reshape(32, D)
    a = jnp.concatenate([w1[:W1A], tx[:TX], w2[:W2A]], axis=0)
    b = jnp.concatenate([w1[W1A:], tx[TX:], w2[W2A:]], axis=0)

    a1, a2 = small_ring(a, W1A + TX, XS)
    b1, b2 = small_ring(b, W1B + TX, "y")
    a1, b1 = large_ring(a1, "y"), large_ring(b1, XS)
    a2, b2 = large_ring(a2, "y"), large_ring(b2, XS)

    normed, own_rows = pl.pallas_call(
        norm_kernel,
        out_shape=(jax.ShapeDtypeStruct((1024, D), BF), jax.ShapeDtypeStruct((512, D), BF)),
        in_specs=[ANY, VM],
        out_specs=(VM, VM),
        scratch_shapes=[pltpu.SemaphoreType.DMA],
        name="norm",
        cost_estimate=pl.CostEstimate(flops=20 * 1024 * D, transcendentals=0, bytes_accessed=6 << 20),
        compiler_params=pltpu.CompilerParams(vmem_limit_bytes=8 << 20),
    )(picture_skip_activations, normaliser_multipliers[0:1])

    cost = pl.CostEstimate(flops=4 * 1024 * D * HID, transcendentals=0, bytes_accessed=12 << 20)
    units, texts = pl.pallas_call(
        widen_kernel,
        out_shape=(jax.ShapeDtypeStruct((2, 1024, HID), BF), jax.ShapeDtypeStruct((PAIRS, D), BF)),
        in_specs=[VM] * 11,
        out_specs=(VM, VM),
        scratch_shapes=[pltpu.VMEM((2, D, HID), BF)],
        name="widen",
        cost_estimate=cost,
        compiler_params=pltpu.CompilerParams(vmem_limit_bytes=14 << 20),
    )(normed, *a1, *b1)
    text_emb = pl.pallas_call(
        text_kernel,
        out_shape=jax.ShapeDtypeStruct((PAIRS, D), BF),
        in_specs=[VM] * 3,
        out_specs=VM,
        name="text",
        cost_estimate=pl.CostEstimate(flops=2 * PAIRS * D * D, transcendentals=0, bytes_accessed=5 << 20),
        compiler_params=pltpu.CompilerParams(vmem_limit_bytes=12 << 20),
    )(normaliser_multipliers[2:3], caption_mapping_matrix, texts)
    units, text_emb = lax.optimization_barrier((units, text_emb))
    half_cost = pl.CostEstimate(flops=2 * 1024 * D * HID, transcendentals=0, bytes_accessed=12 << 20)
    sent, second = pl.pallas_call(
        contract_sent_kernel,
        out_shape=(jax.ShapeDtypeStruct((512, D), BF), jax.ShapeDtypeStruct((2, D, HID), BF)),
        in_specs=[VM] * 11,
        out_specs=(VM, VM),
        name="contract_sent",
        cost_estimate=half_cost,
        compiler_params=pltpu.CompilerParams(vmem_limit_bytes=14 << 20),
    )(units, *a2, *b2)
    received = lax.ppermute(sent, "c", [(0, 1), (1, 0)])
    own = pl.pallas_call(
        contract_own_kernel,
        out_shape=jax.ShapeDtypeStruct((512, D), F32),
        in_specs=[VM, VM],
        out_specs=VM,
        name="contract_own",
        cost_estimate=half_cost,
        compiler_params=pltpu.CompilerParams(vmem_limit_bytes=14 << 20),
    )(units, second)
    message = pl.pallas_call(
        last_kernel,
        out_shape=jax.ShapeDtypeStruct((64, 4, 16), F32),
        in_specs=[SM, SM, VM, VM, VM, VM, VM],
        out_specs=VM,
        name="losses",
        compiler_params=pltpu.CompilerParams(vmem_limit_bytes=12 << 20),
    )(sharpness_factor, score_offset_term, own_rows, own, received, normaliser_multipliers[1:2], text_emb)
    arrived = jnp.sum(lax.all_to_all(message.reshape(256, 16), ALL, 0, 0, tiled=True), axis=0)
    return arrived[8:], arrived[:8]


def solution(mesh):
    finer = Mesh(mesh.devices.reshape(4, 2, 8, 2, 2), ALL)
    dp, mp = DP, ("xl", "c")
    in_specs = (P(dp, None), P(dp, None), P(), P(dp, mp), P(mp, dp), P(), P(), P())
    out_specs = (P(dp), P(dp))

    return jax.shard_map(on_device, mesh=finer, in_specs=in_specs, out_specs=out_specs, check_vma=False)
```

```python
import jax
import jax.numpy as jnp
from jax import lax
from jax.experimental import pallas as pl
from jax.experimental.pallas import tpu as pltpu
from jax.sharding import Mesh
from jax.sharding import PartitionSpec as P


D = 1152
HID = 1152
PATCHES = 256
PAIRS = 512
DP = ("y", "xh", "z")
XS = ("xh", "xl")
ALL = ("y", "xh", "z", "xl", "c")
W1A, W1B, W2A, W2B, TX = 80, 64, 64, 80, 8
BF = jnp.bfloat16
F32 = jnp.float32


def shifted(array, axes, by, size=4):
    return lax.ppermute(array, axes, [(i, (i + by) % size) for i in range(size)])


def small_ring(block, cut, axes):
    right, left = shifted(block, axes, 1), shifted(block, axes, -1)
    far1, far2 = shifted(right[:cut], axes, 1), shifted(left[cut:], axes, -1)
    first = jnp.stack([block[:cut], right[:cut], far1, left[:cut]])
    return first, jnp.stack([block[cut:], right[cut:], far2, left[cut:]])


def large_ring(block, axes):
    right = shifted(block, axes, 1)
    left = shifted(block, axes, -1)
    far_r = shifted(right[:2], axes, 1)
    far_l = shifted(left[2:], axes, -1)
    return block, right, left, far_r, far_l


def gathered_along_z(block):
    one_r, one_l = shifted(block, "z", 1, 8), shifted(block, "z", -1, 8)
    two_r, two_l = shifted(block, "z", 2, 8), shifted(block, "z", -2, 8)
    three_r, three_l = shifted(two_r, "z", 1, 8), shifted(two_l, "z", -1, 8)
    four = shifted(two_r, "z", 2, 8)
    z = lax.axis_index("z")
    out = jnp.zeros((8, *block.shape), block.dtype)
    pieces = ((0, block), (-1, one_r), (1, one_l), (-2, two_r), (2, two_l), (-3, three_r), (3, three_l), (4, four))
    for by, piece in pieces:
        out = lax.dynamic_update_slice(out, piece[None], (lax.rem(z + by + 8, 8), 0, 0))
    return out


def layer_norm(values, norm_gain):
    average = jnp.mean(values, axis=-1, keepdims=True)
    centred = values - average
    spread = jnp.mean(centred * centred, axis=-1, keepdims=True)
    return centred * lax.rsqrt(spread + 1e-06) * norm_gain


def place():
    x = lax.axis_index("xh") * 2 + lax.axis_index("xl")
    return x, lax.axis_index("y")


def each_piece(a_refs, b_refs, write):
    x, y = place()

    def visit(ref, n, i, j, half):
        xk, yk = (i, j) if half == 0 else (j, i)
        write(half, ref, n, lax.rem(x - xk + 4, 4), lax.rem(y - yk + 4, 4))

    def whole(i, _):
        for half, refs in enumerate((a_refs, b_refs)):
            for ref, j in ((refs[0], 0), (refs[1], 1), (refs[2], 3)):
                visit(ref, i, i, j, half)
        return 0

    def halves(u, _):
        for half, refs in enumerate((a_refs, b_refs)):
            visit(refs[3], u, u, 2, half)
            visit(refs[4], u, u + 2, 2, half)
        return 0

    lax.fori_loop(0, 4, whole, 0)
    lax.fori_loop(0, 2, halves, 0)


def put_in_order(rows, dst, ref, half, n, xx, yy):
    at = pl.multiple_of((yy * 2 + xx // 2) * 144 + half * rows[0], 16)
    dst[lax.rem(xx, 2), pl.ds(at, rows[half]), :] = ref[n, 0 : rows[half], :]


ROWS = 512


def gelu(v):
    inner = 0.7978845608028654 * (v + 0.044715 * (v * v * v))
    return (0.5 * v * (1.0 + jnp.tanh(inner))).astype(BF)


def norm_kernel(x_ref, gain_ref, normed_ref, own_ref):
    first = pl.multiple_of(lax.axis_index("xl") * 1024, 1024)
    half = pl.multiple_of(first + lax.axis_index("c") * 512, 512)
    gain = gain_ref[...]

    def keep(r, _):
        rows = pl.multiple_of(r * 64, 64)
        own_ref[pl.ds(rows, 64), :] = x_ref[pl.ds(half + rows, 64), :]
        return 0

    def norm(r, _):
        rows = pl.multiple_of(r * 64, 64)
        values = x_ref[pl.ds(first + rows, 64), :].astype(F32)
        normed_ref[pl.ds(rows, 64), :] = layer_norm(values, gain).astype(BF)
        return 0

    lax.fori_loop(0, 8, keep, 0)
    lax.fori_loop(0, 16, norm, 0)


def widen_kernel(normed_ref, *refs):
    a_refs, b_refs, (h, texts, w1) = refs[:5], refs[5:10], refs[10:]
    rows = (W1A, W1B)

    def write(half, ref, n, xx, yy):
        put_in_order(rows, w1, ref, half, n, xx, yy)
        texts[(yy * 4 + xx) * 2 + half] = ref[n, rows[half] : rows[half] + TX, :]

    each_piece(a_refs, b_refs, write)

    def widen(t, _):
        k = t // 2
        rows = pl.ds(pl.multiple_of(lax.rem(t, 2) * ROWS, ROWS), ROWS)
        h[k, rows, :] = gelu(jnp.dot(normed_ref[rows, :], w1[k], preferred_element_type=F32))
        return 0

    lax.fori_loop(0, 4, widen, 0)


def contracted(h, w2, half, out_ref):
    def step(r, _):
        rows = pl.ds(pl.multiple_of(half * 512 + r * 256, 256), 256)
        total = None
        for k in range(2):
            part = lax.dot_general(
                h[k, rows, :], w2[k], (((1,), (1,)), ((), ())), preferred_element_type=F32
            )
            total = part if total is None else total + part
        out_ref[pl.ds(pl.multiple_of(r * 256, 256), 256), :] = total.astype(out_ref.dtype)
        return 0

    lax.fori_loop(0, 2, step, 0)


def contract_sent_kernel(h, *refs):
    a_refs, b_refs, (sent_ref, w2) = refs[:5], refs[5:10], refs[10:]

    def write(half, ref, n, xx, yy):
        put_in_order((W2A, W2B), w2, ref, half, n, xx, yy)

    each_piece(a_refs, b_refs, write)
    contracted(h, w2, 1 - lax.axis_index("c"), sent_ref)


def contract_own_kernel(h, w2, own_ref):
    contracted(h, w2, lax.axis_index("c"), own_ref)


def text_kernel(gain_ref, map_ref, rows_ref, out_ref):
    gain = gain_ref[...]

    def embed(r, _):
        rows = pl.ds(pl.multiple_of(r * 128, 128), 128)
        normed = layer_norm(rows_ref[rows, :].astype(F32), gain).astype(BF)
        vector = jnp.dot(normed, map_ref[...], preferred_element_type=F32)
        length = jnp.sqrt(jnp.sum(vector * vector, axis=-1, keepdims=True))
        out_ref[rows, :] = (vector / jnp.maximum(length, 1.0)).astype(BF)
        return 0

    lax.fori_loop(0, PAIRS // 256, embed, 0)


def last_kernel(scale_ref, shift_ref, x_ref, own_ref, recv_ref, gain_ref, text_ref, other_ref, out_ref):
    gain = gain_ref[...]
    pooled = []
    for k in range(2):

        def pool(r, total, k=k):
            rows = pl.ds(pl.multiple_of(k * PATCHES + r * 64, 64), 64)
            v = x_ref[rows, :].astype(F32) + (own_ref[rows, :] + recv_ref[rows, :].astype(F32))
            final = layer_norm(v, gain)
            return total + jnp.sum(final.reshape(8, 8, D), axis=0)

        total = lax.fori_loop(0, PATCHES // 64, pool, jnp.zeros((8, D), F32))
        pooled.append(jnp.sum(total, axis=0, keepdims=True) * (1.0 / PATCHES))
    vector = jnp.concatenate(pooled + [jnp.zeros((6, D), F32)], axis=0)
    length = jnp.sqrt(jnp.sum(vector * vector, axis=-1, keepdims=True))
    emb = (vector / jnp.maximum(length, 1.0)).astype(BF)
    scores = jnp.concatenate(
        [
            lax.dot_general(ref[...], emb, (((1,), (1,)), ((), ())), preferred_element_type=F32)
            for ref in (text_ref, other_ref)
        ],
        axis=0,
    )
    scores = scores * scale_ref[0] + shift_ref[0]
    dp = lax.axis_index("y") * 16 + lax.axis_index("xh") * 8 + lax.axis_index("z")
    core = lax.axis_index("c")
    slot = lax.axis_index("xl") * 4 + core * 2
    q = lax.broadcasted_iota(jnp.int32, (PAIRS, 8), 0)
    col = lax.broadcasted_iota(jnp.int32, (PAIRS, 8), 1)
    q_dp = ((q % 256) // 32) * 8 + (q % 16) // 2
    q_slot = ((q // 16) % 2) * 4 + jnp.where(q < 256, core, 1 - core) * 2 + q % 2
    own_pair = (q_dp == dp) & (q_slot == slot + col)
    value = jnp.where(own_pair, -scores, scores)
    terms = jnp.maximum(value, 0.0) + jnp.log1p(jnp.exp(-jnp.abs(value)))
    terms = jnp.where(col < 2, terms, 0.0)
    cols = jnp.sum(terms, axis=1, keepdims=True)
    rows = jnp.sum(terms, axis=0, keepdims=True)
    spread = jnp.where(q_slot == col, cols, 0.0)
    r = lax.broadcasted_iota(jnp.int32, (64, PAIRS), 0)
    c = lax.broadcasted_iota(jnp.int32, (64, PAIRS), 1)
    owner = jnp.where(((c % 256) // 32) * 8 + (c % 16) // 2 == r, 1.0, 0.0)
    col_part = jnp.dot(owner, spread, precision=lax.Precision.HIGHEST, preferred_element_type=F32)
    mr = lax.broadcasted_iota(jnp.int32, (64, 8), 0)
    mc = lax.broadcasted_iota(jnp.int32, (64, 8), 1)
    row_part = jnp.where(mc == slot, rows[:, 0:1], jnp.where(mc == slot + 1, rows[:, 1:2], 0.0))
    row_part = jnp.where(mr == dp, row_part, 0.0)
    message = jnp.concatenate([col_part, row_part], axis=1)
    for m in range(4):
        out_ref[:, m, :] = message


VM = pl.BlockSpec(memory_space=pltpu.VMEM)
SM = pl.BlockSpec(memory_space=pltpu.SMEM)


def on_device(
    picture_skip_activations,
    caption_closing_activations,
    normaliser_multipliers,
    widening_matrix,
    contracting_matrix,
    caption_mapping_matrix,
    sharpness_factor,
    score_offset_term,
):
    first = lax.axis_index("xl") * 4 + lax.axis_index("c") * 2
    texts = lax.dynamic_slice_in_dim(caption_closing_activations, first, 2, 0)
    weights = jnp.concatenate([widening_matrix, contracting_matrix.T], axis=0)
    weights = jnp.pad(weights, ((0, 0), (0, HID - weights.shape[1])))
    shard = jnp.concatenate([weights, texts], axis=0)
    along_z = gathered_along_z(shard)
    w1 = along_z[:, :18].reshape(144, HID)
    w2 = along_z[:, 18:36].reshape(144, HID)
    tx = along_z[:, 36:].reshape(16, D)
    a = jnp.concatenate([w1[:W1A], tx[:TX], w2[:W2A]], axis=0)
    b = jnp.concatenate([w1[W1A:], tx[TX:], w2[W2A:]], axis=0)

    a1, a2 = small_ring(a, W1A + TX, XS)
    b1, b2 = small_ring(b, W1B + TX, "y")
    a1, b1 = large_ring(a1, "y"), large_ring(b1, XS)
    a2, b2 = large_ring(a2, "y"), large_ring(b2, XS)

    normed, own_rows = pl.pallas_call(
        norm_kernel,
        out_shape=(jax.ShapeDtypeStruct((1024, D), BF), jax.ShapeDtypeStruct((512, D), BF)),
        in_specs=[VM, VM],
        out_specs=(VM, VM),
        name="norm",
        cost_estimate=pl.CostEstimate(flops=20 * 1024 * D, transcendentals=0, bytes_accessed=6 << 20),
        compiler_params=pltpu.CompilerParams(vmem_limit_bytes=12 << 20),
    )(picture_skip_activations, normaliser_multipliers[0:1])

    cost = pl.CostEstimate(flops=4 * 1024 * D * HID, transcendentals=0, bytes_accessed=12 << 20)
    units, texts = pl.pallas_call(
        widen_kernel,
        out_shape=(jax.ShapeDtypeStruct((2, 1024, HID), BF), jax.ShapeDtypeStruct((32, TX, D), BF)),
        in_specs=[VM] * 11,
        out_specs=(VM, VM),
        scratch_shapes=[pltpu.VMEM((2, D, HID), BF)],
        name="widen",
        cost_estimate=cost,
        compiler_params=pltpu.CompilerParams(vmem_limit_bytes=14 << 20),
    )(normed, *a1, *b1)
    text_emb = pl.pallas_call(
        text_kernel,
        out_shape=jax.ShapeDtypeStruct((PAIRS // 2, D), BF),
        in_specs=[VM] * 3,
        out_specs=VM,
        name="text",
        cost_estimate=pl.CostEstimate(flops=PAIRS * D * D, transcendentals=0, bytes_accessed=5 << 20),
        compiler_params=pltpu.CompilerParams(vmem_limit_bytes=12 << 20),
    )(normaliser_multipliers[2:3], caption_mapping_matrix, texts.reshape(PAIRS // 2, D))
    other_emb = lax.ppermute(text_emb, "c", [(0, 1), (1, 0)])
    units, text_emb = lax.optimization_barrier((units, text_emb))
    half_cost = pl.CostEstimate(flops=2 * 1024 * D * HID, transcendentals=0, bytes_accessed=12 << 20)
    sent, second = pl.pallas_call(
        contract_sent_kernel,
        out_shape=(jax.ShapeDtypeStruct((512, D), BF), jax.ShapeDtypeStruct((2, D, HID), BF)),
        in_specs=[VM] * 11,
        out_specs=(VM, VM),
        name="contract_sent",
        cost_estimate=half_cost,
        compiler_params=pltpu.CompilerParams(vmem_limit_bytes=14 << 20),
    )(units, *a2, *b2)
    received = lax.ppermute(sent, "c", [(0, 1), (1, 0)])
    own = pl.pallas_call(
        contract_own_kernel,
        out_shape=jax.ShapeDtypeStruct((512, D), F32),
        in_specs=[VM, VM],
        out_specs=VM,
        name="contract_own",
        cost_estimate=half_cost,
        compiler_params=pltpu.CompilerParams(vmem_limit_bytes=14 << 20),
    )(units, second)
    message = pl.pallas_call(
        last_kernel,
        out_shape=jax.ShapeDtypeStruct((64, 4, 16), F32),
        in_specs=[SM, SM] + [VM] * 6,
        out_specs=VM,
        name="losses",
        compiler_params=pltpu.CompilerParams(vmem_limit_bytes=12 << 20),
    )(sharpness_factor, score_offset_term, own_rows, own, received, normaliser_multipliers[1:2], text_emb, other_emb)
    arrived = jnp.sum(lax.all_to_all(message.reshape(256, 16), ALL, 0, 0, tiled=True), axis=0)
    return arrived[8:], arrived[:8]


def solution(mesh):
    finer = Mesh(mesh.devices.reshape(4, 2, 8, 2, 2), ALL)
    dp, mp = DP, ("xl", "c")
    in_specs = (P(dp, None), P(dp, None), P(), P(dp, mp), P(mp, dp), P(), P(), P())
    out_specs = (P(dp), P(dp))

    return jax.shard_map(on_device, mesh=finer, in_specs=in_specs, out_specs=out_specs, check_vma=False)
```
